256 devices in a mesh: gx: 16 (over z, core), gy: 4 (over y), gz: 4 (over x).
Axes of the slice: x: 4, y: 4, z: 8, core: 2. Of those that a mesh axis runs over, the one named last changes fastest.
Arguments:
- queries: bfloat16 [128, 32, 128], P(None, 'gy'), may hold values from -6 to 6
- passages: bfloat16 [8192, 256, 128], P('gx', 'gz'), may hold values from -0.5 to 0.5
- passage_len: int32 [8192], P('gx'), may hold values from 32 to 256
- query_len: int32 [128], replicated, may hold values from 8 to 32
Outputs:
- log_probs: float32 [128, 8192], P(None, ('gx', 'gz'))
The draws below stay inside these ranges and needn't reach their ends.
All inputs are finite; a program needn't handle non-finite values.
Results may differ from the reference program's by a relative error of at most 0.0003.
Values sent between devices are 32-bit elements; how exact they have to be, the bound alone decides.
A program may use at most 64 MiB of HBM per device.

```python
import math
import jax
import jax.numpy as jnp
from jax import lax

DIM = 128
NQ = 128
LQ = 32
LP = 256
NP = 8192


def draw_queries(key, part):
    noise_key = jax.random.fold_in(key, 11)
    values = jnp.clip(jax.random.normal(noise_key, (NQ, LQ, DIM), jnp.float32), -6.0, 6.0)
    return values.astype(jnp.bfloat16)


def draw_passages(key, part):
    noise_key = jax.random.fold_in(key, 21)
    values = jax.random.normal(noise_key, (NP, LP, DIM), jnp.float32) * DIM ** (-0.5)
    values = jnp.clip(values, -0.5, 0.5)
    return values.astype(jnp.bfloat16)


def set_ends(entries, stream_key, smallest, high):
    spot = [jax.random.randint(jax.random.fold_in(stream_key, axis), (), 0, length) for axis, length in enumerate(entries.shape)]
    main_axis = entries.shape.index(max(entries.shape))
    beside = spot[:main_axis] + [(spot[main_axis] + 1) % entries.shape[main_axis]] + spot[main_axis + 1:]
    return entries.at[tuple(spot)].set(smallest).at[tuple(beside)].set(high)


def setup_inputs(seed: int = 0) -> dict:
    arg_keys = jax.random.split(jax.random.key(seed), 5)
    queries = draw_queries(jax.random.fold_in(arg_keys[4], 71), 0)
    passages = draw_passages(jax.random.fold_in(arg_keys[4], 71), 0)
    passage_len = set_ends(jax.random.randint(arg_keys[2], (NP,), LP // 8, LP + 1), jax.random.fold_in(arg_keys[2], 1), LP // 8, LP).astype(jnp.int32)
    query_len = set_ends(jax.random.randint(arg_keys[3], (NQ,), max(1, LQ // 4), LQ + 1), jax.random.fold_in(arg_keys[3], 1), max(1, LQ // 4), LQ).astype(jnp.int32)
    return dict(queries=queries, passages=passages, passage_len=passage_len, query_len=query_len)


masked_low = -1.0e30


def reference(queries, passages, passage_len, query_len):
    flat_queries = queries.reshape(NQ * LQ, DIM)
    per_block = math.gcd(NP, 32)
    num_blocks = NP // per_block
    tile_stack = passages.reshape(num_blocks, per_block * LP, DIM)
    length_stack = passage_len.reshape(num_blocks, per_block)
    query_used = jnp.arange(LQ, dtype=jnp.int32)[None, :] < query_len[:, None]
    token_ids = jnp.arange(LP, dtype=jnp.int32)

    def block_scores(packed):
        passage_tile, tile_len = packed
        scores = jnp.dot(flat_queries, passage_tile.T, preferred_element_type=jnp.float32)
        scores = scores.reshape(NQ * LQ, per_block, LP)
        usable = token_ids[None, :] < tile_len[:, None]
        scores = jnp.where(usable[None], scores, masked_low)
        maxima = jnp.max(scores, axis=2).reshape(NQ, LQ, per_block)
        return jnp.sum(jnp.where(query_used[:, :, None], maxima, 0.0), axis=1)

    pieces = lax.map(block_scores, (tile_stack, length_stack))
    maxsim = jnp.transpose(pieces, (1, 0, 2)).reshape(NQ, NP)
    highest = jnp.max(maxsim, axis=1, keepdims=True)
    summed = jnp.sum(jnp.exp(maxsim - highest), axis=1, keepdims=True)
    return maxsim - (highest + jnp.log(summed))
```

```python
import jax
import jax.numpy as jnp
from jax import lax
from jax.experimental import pallas as pl
from jax.experimental.pallas import tpu as pltpu
from jax.sharding import PartitionSpec as P

masked_low = -1e30
MESH = pl.DeviceIdType.MESH

CHUNK = 32
SHARE = 4
ROWS = 8
TILE = 256


def place(step):
    far, near = (step % 2) * 2 + (step // 2) % 2, step - SHARE
    way, joined, turn = near % 2, (near // 2) % 2, near // 4
    near_piece = turn + 2 * ((way + joined + 1) % 2)
    is_near = jnp.logical_and(step >= SHARE, step < 3 * SHARE)
    offset = jnp.where(step < SHARE, 2, jnp.where(is_near, 1 + 2 * way, 0))
    return offset, jnp.where(is_near, near_piece, far)


def body(
    length_ref, query_ref, count_ref, passages_ref, out_ref,
    held, usable, weights, wide, parts, relay, final, sums, near_stat, far_stat,
    load_sem, relay_sem, final_sem, sums_sem, near_sem, far_sem,
):
    gx, gy, gz = lax.axis_index("gx"), lax.axis_index("gy"), lax.axis_index("gz")
    steps = 4 * SHARE
    tokens, width = passages_ref.shape[1:]
    queries = query_ref.shape[0]

    def load(step):
        offset, piece = place(step)
        start = lax.rem(gz + offset, 4) * (SHARE * CHUNK) + piece * CHUNK
        return pltpu.make_async_copy(
            passages_ref.at[pl.ds(start, CHUNK)], held.at[step], load_sem.at[step]
        )

    for step in range(steps):
        load(jnp.int32(step)).start()

    barrier = pltpu.get_barrier_semaphore()
    for axis, size, here in (("gz", 4, gz), ("gy", 4, gy), ("gx", 16, gx)):
        for k in range(1, size):
            pl.semaphore_signal(
                barrier, inc=1, device_id={axis: lax.rem(here + k, size)}, device_id_type=MESH
            )

    wide[...] = query_ref[...].reshape(queries * ROWS, width).astype(jnp.float32)
    for i in range(ROWS):
        row = wide[pl.ds(i, queries, stride=ROWS), :]
        weights[:, i * queries : (i + 1) * queries] = row.T.astype(jnp.bfloat16)

    sublane = lax.broadcasted_iota(jnp.int32, (8, TILE), 0)
    odd = [(sublane & k) != 0 for k in (1, 2, 4)]
    token = lax.broadcasted_iota(jnp.int32, (tokens, width), 0)

    def relay_copy(way, turn, source):
        return pltpu.make_async_remote_copy(
            src_ref=source, dst_ref=relay.at[way, turn],
            send_sem=relay_sem.at[0, way, turn], recv_sem=relay_sem.at[1, way, turn],
            device_id={"gz": lax.rem(gz + 1 + 2 * way, 4)}, device_id_type=MESH,
        )

    def final_copy(way, piece, source):
        return pltpu.make_async_remote_copy(
            src_ref=source, dst_ref=final.at[way, piece],
            send_sem=final_sem.at[0, way, piece], recv_sem=final_sem.at[1, way, piece],
            device_id={"gz": lax.rem(gz + 1 + 2 * way, 4)}, device_id_type=MESH,
        )

    def sums_copy(k, piece):
        return pltpu.make_async_remote_copy(
            src_ref=sums.at[gy, piece], dst_ref=sums.at[gy, piece],
            send_sem=sums_sem.at[0, k, piece], recv_sem=sums_sem.at[1, k, piece],
            device_id={"gy": lax.rem(gy + k, 4)}, device_id_type=MESH,
        )

    def near_copy(k):
        return pltpu.make_async_remote_copy(
            src_ref=near_stat.at[gz], dst_ref=near_stat.at[gz],
            send_sem=near_sem.at[0, k], recv_sem=near_sem.at[1, k],
            device_id={"gz": lax.rem(gz + k, 4)}, device_id_type=MESH,
        )

    def far_copy(k):
        return pltpu.make_async_remote_copy(
            src_ref=far_stat.at[gx], dst_ref=far_stat.at[gx],
            send_sem=far_sem.at[0, k], recv_sem=far_sem.at[1, k],
            device_id={"gx": lax.rem(gx + k, 16)}, device_id_type=MESH,
        )

    def score(step):
        offset, piece = place(step)
        start = lax.rem(gz + offset, 4) * (SHARE * CHUNK) + piece * CHUNK
        load(step).wait()
        for half in range(CHUNK // 8):
            some = jnp.zeros((8, TILE), jnp.int32)
            for p in range(half * 8, half * 8 + 8):
                used = length_ref[start + p] - gz * tokens
                some = jnp.where(sublane == p % 8, used, some)
                block = held[step, p].astype(jnp.float32)
                block = jnp.where(token < used, block, block[0:1])
                usable[p * tokens : (p + 1) * tokens] = block.astype(jnp.bfloat16)
            any_used = some > 0
            for t in range(ROWS * queries // TILE):
                scores = jnp.dot(
                    usable[half * 8 * tokens : (half + 1) * 8 * tokens],
                    weights[:, t * TILE : (t + 1) * TILE],
                    preferred_element_type=jnp.float32,
                )
                best = []
                for p in range(8):
                    rows = [
                        scores[p * tokens + k : p * tokens + k + 8] for k in range(0, tokens, 8)
                    ]
                    while len(rows) > 1:
                        rows = [jnp.maximum(*rows[k : k + 2]) for k in range(0, len(rows), 2)]
                    best.append(rows[0])
                for level, mask in enumerate(odd):
                    best = [
                        jnp.maximum(
                            jnp.where(mask, b, a),
                            pltpu.roll(jnp.where(mask, a, b), 1 << level, 0),
                        )
                        for a, b in zip(best[::2], best[1::2])
                    ]
                result = jnp.where(any_used, best[0], masked_low)
                for side in range(TILE // queries):
                    parts[step, t * (TILE // queries) + side, half * 8 : half * 8 + 8] = result[
                        :, side * queries : (side + 1) * queries
                    ]

    def one_step(step, carry):
        score(step)

        @pl.when(step == 0)
        def _():
            pl.semaphore_wait(barrier, 21)

        @pl.when(step < SHARE)
        def _():
            relay_copy(step % 2, step // 2, parts.at[step]).start()

        @pl.when(jnp.logical_and(step >= SHARE, step < 3 * SHARE))
        def _():
            near = step - SHARE
            way, joined, turn = near % 2, (near // 2) % 2, near // 4

            @pl.when(joined == 1)
            def _():
                relay_copy(way, turn, parts.at[step]).wait_recv()
                parts[step] = jnp.maximum(parts[step], relay[way, turn])

            final_copy(way, place(step)[1], parts.at[step]).start()

        @pl.when(step >= 3 * SHARE)
        def _():
            piece = place(step)[1]
            for way in range(2):
                final_copy(way, piece, parts.at[step]).wait_recv()
            total = jnp.zeros((CHUNK, queries), jnp.float32)
            for i in range(ROWS):
                best = jnp.maximum(
                    parts[step, i], jnp.maximum(final[0, piece, i], final[1, piece, i])
                )
                total = total + jnp.where(gy * ROWS + i < count_ref[...], best, 0.0)
            sums[gy, piece] = total
            for k in range(1, 4):
                sums_copy(k, piece).start()

        return carry

    lax.fori_loop(0, steps, one_step, 0)

    for piece in range(SHARE):
        for k in range(1, 4):
            sums_copy(k, piece).wait_recv()
    maxsim = (sums[0] + sums[1]) + (sums[2] + sums[3])
    maxsim = maxsim.reshape(SHARE * CHUNK, queries)

    def joined_stats(stats):
        top = jnp.max(stats, axis=0, keepdims=True)
        return top + jnp.log(jnp.sum(jnp.exp(stats - top), axis=0, keepdims=True))

    near_stat[gz] = joined_stats(maxsim)
    for k in range(1, 4):
        near_copy(k).start()
    for k in range(1, 4):
        near_copy(k).wait_recv()
    far_stat[gx] = joined_stats(near_stat[...].reshape(4, queries))
    for k in range(1, 16):
        far_copy(k).start()
    for k in range(1, 16):
        far_copy(k).wait_recv()
    norm = joined_stats(far_stat[...].reshape(16, queries))
    out_ref[...] = (maxsim - norm).T

    for way in range(2):
        for turn in range(2):
            relay_copy(way, turn, parts.at[0]).wait_send()
        for piece in range(SHARE):
            final_copy(way, piece, parts.at[0]).wait_send()
    for k in range(1, 4):
        for piece in range(SHARE):
            sums_copy(k, piece).wait_send()
        near_copy(k).wait_send()
    for k in range(1, 16):
        far_copy(k).wait_send()


def shards(queries, passages, passage_len, query_len):
    count, rows, width = queries.shape
    tokens = passages.shape[1]
    f32 = jnp.float32
    vmem = pl.BlockSpec(memory_space=pltpu.VMEM)
    return pl.pallas_call(
        body,
        out_shape=jax.ShapeDtypeStruct((count, SHARE * CHUNK), f32),
        in_specs=[
            pl.BlockSpec(memory_space=pltpu.SMEM), vmem, vmem, pl.BlockSpec(memory_space=pl.ANY)
        ],
        out_specs=vmem,
        scratch_shapes=[
            pltpu.VMEM((4 * SHARE, CHUNK, tokens, width), jnp.bfloat16),
            pltpu.VMEM((CHUNK * tokens, width), jnp.bfloat16),
            pltpu.VMEM((width, rows * count), jnp.bfloat16),
            pltpu.VMEM((rows * count, width), f32),
            pltpu.VMEM((4 * SHARE, rows, CHUNK, count), f32),
            pltpu.VMEM((2, 2, rows, CHUNK, count), f32),
            pltpu.VMEM((2, SHARE, rows, CHUNK, count), f32),
            pltpu.VMEM((4, SHARE, CHUNK, count), f32),
            pltpu.VMEM((4, 1, count), f32),
            pltpu.VMEM((16, 1, count), f32),
            pltpu.SemaphoreType.DMA((4 * SHARE,)),
            pltpu.SemaphoreType.DMA((2, 2, 2)),
            pltpu.SemaphoreType.DMA((2, 2, SHARE)),
            pltpu.SemaphoreType.DMA((2, 4, SHARE)),
            pltpu.SemaphoreType.DMA((2, 4)),
            pltpu.SemaphoreType.DMA((2, 16)),
        ],
        compiler_params=pltpu.CompilerParams(
            collective_id=0, has_side_effects=True, vmem_limit_bytes=60 * 2**20
        ),
        name="late_interaction",
    )(passage_len, queries, query_len.reshape(1, count), passages)


def solution(mesh):
    return jax.shard_map(
        shards,
        mesh=mesh,
        in_specs=(P(None, "gy", None), P("gx", "gz", None), P("gx"), P()),
        out_specs=P(None, ("gx", "gz")),
        check_vma=False,
    )
```

```python
import functools

import jax
import jax.numpy as jnp
from jax import lax
from jax.experimental import pallas as pl
from jax.experimental.pallas import tpu as pltpu
from jax.sharding import PartitionSpec as P

masked_low = -1e30
MESH = pl.DeviceIdType.MESH

CHUNK = 32
SHARE = 4
ROWS = 8
TILE = 256
TILES = 3
FOREIGN = 3
FIT_THIRD, FIT_LAST = 640, 384


def place(step):
    far, near = (step % 2) * 2 + (step // 2) % 2, step - SHARE
    way, joined, turn = near % 2, (near // 2) % 2, near // 4
    near_piece = turn + 2 * ((way + joined + 1) % 2)
    is_near = jnp.logical_and(step >= SHARE, step < 3 * SHARE)
    offset = jnp.where(step < SHARE, 2, jnp.where(is_near, 1 + 2 * way, 0))
    return offset, jnp.where(is_near, near_piece, far)


def plain_body(
    length_ref, query_ref, count_ref, passages_ref, out_ref,
    held, usable, weights, wide, parts, relay, final, sums, near_stat, far_stat,
    load_sem, relay_sem, final_sem, sums_sem, near_sem, far_sem,
):
    gx, gy, gz = lax.axis_index("gx"), lax.axis_index("gy"), lax.axis_index("gz")
    steps = 4 * SHARE
    tokens, width = passages_ref.shape[1:]
    queries = query_ref.shape[0]

    def load(step):
        offset, piece = place(step)
        start = lax.rem(gz + offset, 4) * (SHARE * CHUNK) + piece * CHUNK
        return pltpu.make_async_copy(
            passages_ref.at[pl.ds(start, CHUNK)], held.at[step], load_sem.at[step]
        )

    for step in range(steps):
        load(jnp.int32(step)).start()

    barrier = pltpu.get_barrier_semaphore()
    for axis, size, here in (("gz", 4, gz), ("gy", 4, gy), ("gx", 16, gx)):
        for k in range(1, size):
            pl.semaphore_signal(
                barrier, inc=1, device_id={axis: lax.rem(here + k, size)}, device_id_type=MESH
            )

    wide[...] = query_ref[...].reshape(queries * ROWS, width).astype(jnp.float32)
    for i in range(ROWS):
        row = wide[pl.ds(i, queries, stride=ROWS), :]
        weights[:, i * queries : (i + 1) * queries] = row.T.astype(jnp.bfloat16)

    sublane = lax.broadcasted_iota(jnp.int32, (8, TILE), 0)
    odd = [(sublane & k) != 0 for k in (1, 2, 4)]
    token = lax.broadcasted_iota(jnp.int32, (tokens, width), 0)

    def relay_copy(way, turn, source):
        return pltpu.make_async_remote_copy(
            src_ref=source, dst_ref=relay.at[way, turn],
            send_sem=relay_sem.at[0, way, turn], recv_sem=relay_sem.at[1, way, turn],
            device_id={"gz": lax.rem(gz + 1 + 2 * way, 4)}, device_id_type=MESH,
        )

    def final_copy(way, piece, source):
        return pltpu.make_async_remote_copy(
            src_ref=source, dst_ref=final.at[way, piece],
            send_sem=final_sem.at[0, way, piece], recv_sem=final_sem.at[1, way, piece],
            device_id={"gz": lax.rem(gz + 1 + 2 * way, 4)}, device_id_type=MESH,
        )

    def sums_copy(k, piece):
        return pltpu.make_async_remote_copy(
            src_ref=sums.at[gy, piece], dst_ref=sums.at[gy, piece],
            send_sem=sums_sem.at[0, k, piece], recv_sem=sums_sem.at[1, k, piece],
            device_id={"gy": lax.rem(gy + k, 4)}, device_id_type=MESH,
        )

    def near_copy(k):
        return pltpu.make_async_remote_copy(
            src_ref=near_stat.at[gz], dst_ref=near_stat.at[gz],
            send_sem=near_sem.at[0, k], recv_sem=near_sem.at[1, k],
            device_id={"gz": lax.rem(gz + k, 4)}, device_id_type=MESH,
        )

    def far_copy(k):
        return pltpu.make_async_remote_copy(
            src_ref=far_stat.at[gx], dst_ref=far_stat.at[gx],
            send_sem=far_sem.at[0, k], recv_sem=far_sem.at[1, k],
            device_id={"gx": lax.rem(gx + k, 16)}, device_id_type=MESH,
        )

    def score(step):
        offset, piece = place(step)
        start = lax.rem(gz + offset, 4) * (SHARE * CHUNK) + piece * CHUNK
        load(step).wait()
        for half in range(CHUNK // 8):
            some = jnp.zeros((8, TILE), jnp.int32)
            for p in range(half * 8, half * 8 + 8):
                used = length_ref[start + p] - gz * tokens
                some = jnp.where(sublane == p % 8, used, some)
                block = held[step, p].astype(jnp.float32)
                block = jnp.where(token < used, block, block[0:1])
                usable[p * tokens : (p + 1) * tokens] = block.astype(jnp.bfloat16)
            any_used = some > 0
            for t in range(ROWS * queries // TILE):
                scores = jnp.dot(
                    usable[half * 8 * tokens : (half + 1) * 8 * tokens],
                    weights[:, t * TILE : (t + 1) * TILE],
                    preferred_element_type=jnp.float32,
                )
                best = []
                for p in range(8):
                    rows = [
                        scores[p * tokens + k : p * tokens + k + 8] for k in range(0, tokens, 8)
                    ]
                    while len(rows) > 1:
                        rows = [jnp.maximum(*rows[k : k + 2]) for k in range(0, len(rows), 2)]
                    best.append(rows[0])
                for level, mask in enumerate(odd):
                    best = [
                        jnp.maximum(
                            jnp.where(mask, b, a),
                            pltpu.roll(jnp.where(mask, a, b), 1 << level, 0),
                        )
                        for a, b in zip(best[::2], best[1::2])
                    ]
                result = jnp.where(any_used, best[0], masked_low)
                for side in range(TILE // queries):
                    parts[step, t * (TILE // queries) + side, half * 8 : half * 8 + 8] = result[
                        :, side * queries : (side + 1) * queries
                    ]

    def one_step(step, carry):
        score(step)

        @pl.when(step == 0)
        def _():
            pl.semaphore_wait(barrier, 21)

        @pl.when(step < SHARE)
        def _():
            relay_copy(step % 2, step // 2, parts.at[step]).start()

        @pl.when(jnp.logical_and(step >= SHARE, step < 3 * SHARE))
        def _():
            near = step - SHARE
            way, joined, turn = near % 2, (near // 2) % 2, near // 4

            @pl.when(joined == 1)
            def _():
                relay_copy(way, turn, parts.at[step]).wait_recv()
                parts[step] = jnp.maximum(parts[step], relay[way, turn])

            final_copy(way, place(step)[1], parts.at[step]).start()

        @pl.when(step >= 3 * SHARE)
        def _():
            piece = place(step)[1]
            for way in range(2):
                final_copy(way, piece, parts.at[step]).wait_recv()
            total = jnp.zeros((CHUNK, queries), jnp.float32)
            for i in range(ROWS):
                best = jnp.maximum(
                    parts[step, i], jnp.maximum(final[0, piece, i], final[1, piece, i])
                )
                total = total + jnp.where(gy * ROWS + i < count_ref[...], best, 0.0)
            sums[gy, piece] = total
            for k in range(1, 4):
                sums_copy(k, piece).start()

        return carry

    lax.fori_loop(0, steps, one_step, 0)

    for piece in range(SHARE):
        for k in range(1, 4):
            sums_copy(k, piece).wait_recv()
    maxsim = (sums[0] + sums[1]) + (sums[2] + sums[3])
    maxsim = maxsim.reshape(SHARE * CHUNK, queries)

    def joined_stats(stats):
        top = jnp.max(stats, axis=0, keepdims=True)
        return top + jnp.log(jnp.sum(jnp.exp(stats - top), axis=0, keepdims=True))

    near_stat[gz] = joined_stats(maxsim)
    for k in range(1, 4):
        near_copy(k).start()
    for k in range(1, 4):
        near_copy(k).wait_recv()
    far_stat[gx] = joined_stats(near_stat[...].reshape(4, queries))
    for k in range(1, 16):
        far_copy(k).start()
    for k in range(1, 16):
        far_copy(k).wait_recv()
    norm = joined_stats(far_stat[...].reshape(16, queries))
    out_ref[...] = (maxsim - norm).T

    for way in range(2):
        for turn in range(2):
            relay_copy(way, turn, parts.at[0]).wait_send()
        for piece in range(SHARE):
            final_copy(way, piece, parts.at[0]).wait_send()
    for k in range(1, 4):
        for piece in range(SHARE):
            sums_copy(k, piece).wait_send()
        near_copy(k).wait_send()
    for k in range(1, 16):
        far_copy(k).wait_send()


def packed_body(
    length_ref, query_ref, count_ref, passages_ref, out_ref,
    held, raw, choice, owner, weights, wide, given, foreign, far_parts, parts, relay, final,
    sums, near_stat, far_stat,
    load_sem, given_sem, relay_sem, final_sem, sums_sem, near_sem, far_sem,
):
    gx, gy, gz = lax.axis_index("gx"), lax.axis_index("gy"), lax.axis_index("gz")
    tokens, width = passages_ref.shape[1:]
    queries = query_ref.shape[0]
    f32, bf16 = jnp.float32, jnp.bfloat16
    half_share = SHARE * CHUNK // 2
    core = lax.rem(gx, 2)
    slot = core * 4 + gz

    def start_of(share, piece):
        offset = jnp.where(share == 0, 2, jnp.where(share == 3, 0, 2 * share - 1))
        return lax.rem(gz + offset, 4) * (SHARE * CHUNK) + piece * CHUNK

    def load(share, piece):
        return pltpu.make_async_copy(
            passages_ref.at[pl.ds(start_of(share, piece), CHUNK)],
            held.at[share * SHARE + piece], load_sem.at[share * SHARE + piece],
        )

    def near_place(n):
        way, joined, turn = n % 2, (n // 2) % 2, n // 4
        own = n >= 8
        piece = jnp.where(own, way * 2 + joined, turn + 2 * ((way + joined + 1) % 2))
        return jnp.where(own, 3, 1 + way), piece

    for piece in range(SHARE):
        load(jnp.int32(0), piece).start()
    for n in range(12):
        load(*near_place(jnp.int32(n))).start()

    def near_peer(k):
        to_core = lax.rem(core + k // 4, 2)
        return {"gx": gx - core + to_core, "gz": lax.rem(gz + k % 4, 4)}

    barrier = pltpu.get_barrier_semaphore()
    peers = [{"gy": lax.rem(gy + k, 4)} for k in range(1, 4)]
    peers += [near_peer(k) for k in range(1, 8)]
    peers += [{"gx": lax.rem(gx + 2 * k, 16)} for k in range(1, 8)]
    foreign[...] = jnp.zeros(foreign.shape, f32)
    for peer in peers:
        pl.semaphore_signal(barrier, inc=1, device_id=peer, device_id_type=MESH)

    def given_copy(k, target, to):
        return pltpu.make_async_remote_copy(
            src_ref=given.at[k], dst_ref=foreign.at[target],
            send_sem=given_sem.at[0, k], recv_sem=given_sem.at[1, target],
            device_id={"gy": to}, device_id_type=MESH,
        )

    def relay_copy(way, tile):
        return pltpu.make_async_remote_copy(
            src_ref=far_parts.at[tile, way], dst_ref=relay.at[way, tile],
            send_sem=relay_sem.at[0, way, tile], recv_sem=relay_sem.at[1, way, tile],
            device_id={"gz": lax.rem(gz + 1 + 2 * way, 4)}, device_id_type=MESH,
        )

    def final_copy(way, piece, source):
        return pltpu.make_async_remote_copy(
            src_ref=source, dst_ref=final.at[way, piece],
            send_sem=final_sem.at[0, way, piece], recv_sem=final_sem.at[1, way, piece],
            device_id={"gz": lax.rem(gz + 1 + 2 * way, 4)}, device_id_type=MESH,
        )

    def sums_copy(k, piece):
        return pltpu.make_async_remote_copy(
            src_ref=sums.at[gy, piece], dst_ref=sums.at[gy, piece],
            send_sem=sums_sem.at[0, k, piece], recv_sem=sums_sem.at[1, k, piece],
            device_id={"gy": lax.rem(gy + k, 4)}, device_id_type=MESH,
        )

    def near_copy(k):
        return pltpu.make_async_remote_copy(
            src_ref=near_stat.at[slot], dst_ref=near_stat.at[slot],
            send_sem=near_sem.at[0, k], recv_sem=near_sem.at[1, k],
            device_id=near_peer(k), device_id_type=MESH,
        )

    def far_copy(k):
        return pltpu.make_async_remote_copy(
            src_ref=far_stat.at[gx // 2], dst_ref=far_stat.at[gx // 2],
            send_sem=far_sem.at[0, k], recv_sem=far_sem.at[1, k],
            device_id={"gx": lax.rem(gx + 2 * k, 16)}, device_id_type=MESH,
        )

    wide[...] = query_ref[...].reshape(queries * ROWS, width).astype(f32)
    given[0] = wide[pl.ds(ROWS - 2, queries, stride=ROWS), :]
    given[1] = wide[pl.ds(ROWS - 1, queries, stride=ROWS), :]

    @pl.when(gy < 2)
    def _():
        pl.semaphore_wait(barrier, 17)

    @pl.when(gy == 0)
    def _():
        given_copy(0, 0, 3).start()
        given_copy(1, 1, 3).start()

    @pl.when(gy == 1)
    def _():
        given_copy(1, 2, 3).start()
        given_copy(0, 0, 2).start()

    for i in range(ROWS):
        row = wide[pl.ds(i, queries, stride=ROWS), :]
        raw[:, i * queries : (i + 1) * queries] = row.T.astype(bf16)

    lane = lax.broadcasted_iota(jnp.int32, (queries, 128), 1)
    line = lax.broadcasted_iota(jnp.int32, (queries, 128), 0)
    token_of = jnp.where(lane < ROWS, gy * ROWS + lane, 99)
    token_of = jnp.where(jnp.logical_and(gy < 2, lane >= ROWS - 2), 99, token_of)
    token_of = jnp.where(jnp.logical_and(gy == 2, lane == ROWS), 14, token_of)
    for k, token in enumerate((6, 7, 15)):
        token_of = jnp.where(jnp.logical_and(gy == 3, lane == ROWS + k), token, token_of)
    lengths = jnp.broadcast_to(count_ref[...].astype(f32), (queries, 128)).T
    valid = token_of.astype(f32) < lengths
    one = jnp.where(valid, 1.0, 0.0).astype(bf16)
    below = jnp.where(lane < line, 1.0, 0.0).astype(bf16)
    above = jnp.where(line < lane, 1.0, 0.0).astype(bf16)
    rank = jnp.dot(below, one, preferred_element_type=f32)
    earlier = jnp.dot(one, above, preferred_element_type=f32).astype(bf16)
    base = jnp.dot(jnp.ones((queries, 128), bf16), earlier, preferred_element_type=f32)
    gap = jnp.maximum(TILE - base[:, ROWS : ROWS + 1], 0.0)
    place_of = rank + base + jnp.where(lane >= ROWS, gap, 0.0)
    place_of = jnp.where(valid, place_of, -1.0)
    lane_wide = lax.broadcasted_iota(jnp.int32, (queries, TILE), 1).astype(f32)

    def pack(tile):
        slots = ROWS if tile == 0 else ROWS + FOREIGN
        taken = jnp.zeros((queries, TILE), f32)
        for s in range(slots):
            hit = jnp.where(place_of[:, s : s + 1] == lane_wide + float(tile * TILE), 1.0, 0.0)
            taken = taken + hit
            choice[s * queries : (s + 1) * queries] = hit.astype(bf16)
        owner[tile] = taken.astype(bf16)
        weights[tile] = jnp.dot(
            raw[:, : slots * queries], choice[: slots * queries], preferred_element_type=f32
        ).astype(bf16)

    sublane = lax.broadcasted_iota(jnp.int32, (8, TILE), 0)
    odd = [(sublane & k) != 0 for k in (1, 2, 4)]
    token = lax.broadcasted_iota(jnp.int32, (tokens, width), 0)

    def score(index, start, fix, tiles, put):
        for eighth in range(CHUNK // 8):
            some = jnp.zeros((8, TILE), jnp.int32)
            for p in range(eighth * 8, eighth * 8 + 8):
                used = length_ref[start + p] - gz * tokens
                some = jnp.where(sublane == p % 8, used, some)
                if fix:
                    block = held[index, p].astype(f32)
                    held[index, p] = jnp.where(token < used, block, block[0:1]).astype(bf16)
            any_used = some > 0
            block = held[index, eighth * 8 : eighth * 8 + 8].reshape(8 * tokens, width)
            for t in tiles:
                scores = jnp.dot(block, weights[t], preferred_element_type=f32)
                best = []
                for p in range(8):
                    rows = [
                        scores[p * tokens + k : p * tokens + k + 8] for k in range(0, tokens, 8)
                    ]
                    while len(rows) > 1:
                        rows = [jnp.maximum(*rows[k : k + 2]) for k in range(0, len(rows), 2)]
                    best.append(rows[0])
                for level, mask in enumerate(odd):
                    best = [
                        jnp.maximum(
                            jnp.where(mask, b, a),
                            pltpu.roll(jnp.where(mask, a, b), 1 << level, 0),
                        )
                        for a, b in zip(best[::2], best[1::2])
                    ]
                put(t, eighth * 8, jnp.where(any_used, best[0], masked_low))

    for tile in range(TILES):
        if tile == 1:

            @pl.when(gy == 2)
            def _():
                given_copy(0, 0, 2).wait_recv()

            @pl.when(gy == 3)
            def _():
                for k in range(FOREIGN):
                    given_copy(0, k, 3).wait_recv()

            for k in range(FOREIGN):
                raw[:, (ROWS + k) * queries : (ROWS + k + 1) * queries] = foreign[k].T.astype(bf16)
        pack(tile)
        for piece in range(SHARE):
            if tile == 0:
                load(jnp.int32(0), piece).wait()

            def put(t, row, value, piece=piece):
                row = piece % 2 * CHUNK + row
                far_parts[t, piece // 2, row : row + 8] = value

            score(piece, start_of(jnp.int32(0), piece), tile == 0, (tile,), put)
        if tile == 0:

            @pl.when(gy >= 2)
            def _():
                pl.semaphore_wait(barrier, 17)

        for way in range(2):
            relay_copy(way, tile).start()

    def later(n, carry):
        share, piece = near_place(n)
        load(share, piece).wait()

        def put(t, row, value):
            parts[n, t, row : row + 8] = value

        score(share * SHARE + piece, start_of(share, piece), True, range(TILES), put)

        @pl.when(n < 8)
        def _():
            way, joined, turn = n % 2, (n // 2) % 2, n // 4

            @pl.when(jnp.logical_and(joined == 1, turn == 0))
            def _():
                for tile in range(TILES):
                    relay_copy(way, tile).wait_recv()

            @pl.when(joined == 1)
            def _():
                for tile in range(TILES):
                    parts[n, tile] = jnp.maximum(
                        parts[n, tile], relay[way, tile, pl.ds(turn * CHUNK, CHUNK)]
                    )

            final_copy(way, piece, parts.at[n]).start()

        @pl.when(n >= 8)
        def _():
            for way in range(2):
                final_copy(way, piece, parts.at[n]).wait_recv()
            total = jnp.zeros((CHUNK, queries), f32)
            for tile in range(TILES):
                best = jnp.maximum(
                    parts[n, tile], jnp.maximum(final[0, piece, tile], final[1, piece, tile])
                )
                for _ in range(3):
                    term = best.astype(bf16)
                    total = total + lax.dot_general(
                        term, owner[tile], (((1,), (1,)), ((), ())), preferred_element_type=f32
                    )
                    best = best - term.astype(f32)
            sums[gy, piece] = total
            for k in range(1, 4):
                sums_copy(k, piece).start()

        return carry

    lax.fori_loop(0, 12, later, 0)

    for piece in range(SHARE):
        for k in range(1, 4):
            sums_copy(k, piece).wait_recv()
    maxsim = (sums[0] + sums[1]) + (sums[2] + sums[3])
    maxsim = maxsim.reshape(SHARE * CHUNK, queries)

    def joined_stats(stats):
        top = jnp.max(stats, axis=0, keepdims=True)
        return top + jnp.log(jnp.sum(jnp.exp(stats - top), axis=0, keepdims=True))

    near_stat[slot] = joined_stats(maxsim)
    for k in range(1, 8):
        near_copy(k).start()
    for k in range(1, 8):
        near_copy(k).wait_recv()
    far_stat[gx // 2] = joined_stats(near_stat[...].reshape(8, queries))
    for k in range(1, 8):
        far_copy(k).start()
    for k in range(1, 8):
        far_copy(k).wait_recv()
    norm = joined_stats(far_stat[...].reshape(8, queries))
    out_ref[...] = (maxsim - norm).T

    @pl.when(gy < 2)
    def _():
        for k in range(2):
            given_copy(k, 0, 3).wait_send()

    for way in range(2):
        for tile in range(TILES):
            relay_copy(way, tile).wait_send()
        for piece in range(SHARE):
            final_copy(way, piece, parts.at[0]).wait_send()
    for k in range(1, 4):
        for piece in range(SHARE):
            sums_copy(k, piece).wait_send()
    for k in range(1, 8):
        near_copy(k).wait_send()
        far_copy(k).wait_send()


def call(body, name, collective, scratch, lengths, queries, counts, passages):
    vmem = pl.BlockSpec(memory_space=pltpu.VMEM)
    return pl.pallas_call(
        body,
        out_shape=jax.ShapeDtypeStruct((queries.shape[0], SHARE * CHUNK), jnp.float32),
        in_specs=[
            pl.BlockSpec(memory_space=pltpu.SMEM), vmem, vmem, pl.BlockSpec(memory_space=pl.ANY)
        ],
        out_specs=vmem,
        scratch_shapes=scratch,
        compiler_params=pltpu.CompilerParams(
            collective_id=collective, has_side_effects=True, vmem_limit_bytes=60 * 2**20
        ),
        name=name,
    )(lengths, queries, counts, passages)


def shards(queries, passages, passage_len, query_len):
    count, rows, width = queries.shape
    tokens = passages.shape[1]
    f32, bf16 = jnp.float32, jnp.bfloat16
    dma = pltpu.SemaphoreType.DMA
    plain = [
        pltpu.VMEM((4 * SHARE, CHUNK, tokens, width), bf16),
        pltpu.VMEM((CHUNK * tokens, width), bf16),
        pltpu.VMEM((width, rows * count), bf16),
        pltpu.VMEM((rows * count, width), f32),
        pltpu.VMEM((4 * SHARE, rows, CHUNK, count), f32),
        pltpu.VMEM((2, 2, rows, CHUNK, count), f32),
        pltpu.VMEM((2, SHARE, rows, CHUNK, count), f32),
        pltpu.VMEM((4, SHARE, CHUNK, count), f32),
        pltpu.VMEM((4, 1, count), f32),
        pltpu.VMEM((16, 1, count), f32),
        dma((4 * SHARE,)),
        dma((2, 2, 2)),
        dma((2, 2, SHARE)),
        dma((2, 4, SHARE)),
        dma((2, 4)),
        dma((2, 16)),
    ]
    packed = [
        pltpu.VMEM((4 * SHARE, CHUNK, tokens, width), bf16),
        pltpu.VMEM((width, (rows + FOREIGN) * count), bf16),
        pltpu.VMEM(((rows + FOREIGN) * count, TILE), bf16),
        pltpu.VMEM((TILES, count, TILE), bf16),
        pltpu.VMEM((TILES, width, TILE), bf16),
        pltpu.VMEM((rows * count, width), f32),
        pltpu.VMEM((2, count, width), f32),
        pltpu.VMEM((FOREIGN, count, width), f32),
        pltpu.VMEM((TILES, 2, SHARE * CHUNK // 2, TILE), f32),
        pltpu.VMEM((12, TILES, CHUNK, TILE), f32),
        pltpu.VMEM((2, TILES, SHARE * CHUNK // 2, TILE), f32),
        pltpu.VMEM((2, SHARE, TILES, CHUNK, TILE), f32),
        pltpu.VMEM((4, SHARE, CHUNK, count), f32),
        pltpu.VMEM((8, 1, count), f32),
        pltpu.VMEM((8, 1, count), f32),
        dma((4 * SHARE,)),
        dma((2, FOREIGN)),
        dma((2, 2, TILES)),
        dma((2, 2, SHARE)),
        dma((2, 4, SHARE)),
        dma((2, 8)),
        dma((2, 8)),
    ]
    third = jnp.clip(query_len - 2 * rows, 0, rows)
    last = jnp.clip(query_len - 3 * rows, 0, rows)
    counted = jnp.sum(third + last * 4096)
    fits = jnp.logical_and(
        (counted & 4095) <= FIT_THIRD, lax.shift_right_logical(counted, 12) <= FIT_LAST
    )
    return lax.cond(
        fits,
        functools.partial(call, packed_body, "packed_scores", 0, packed),
        functools.partial(call, plain_body, "plain_scores", 1, plain),
        passage_len,
        queries,
        query_len.reshape(1, count),
        passages,
    )


def solution(mesh):
    return jax.shard_map(
        shards,
        mesh=mesh,
        in_specs=(P(None, "gy", None), P("gx", "gz", None), P("gx"), P()),
        out_specs=P(None, ("gx", "gz")),
        check_vma=False,
    )
```

```python
import jax
import jax.numpy as jnp
from jax import lax
from jax.experimental import pallas as pl
from jax.experimental.pallas import tpu as pltpu
from jax.sharding import PartitionSpec as P

masked_low = -1e30
MESH = pl.DeviceIdType.MESH

PIECE = 32
SHARE = 4
HALF = PIECE * SHARE // 2
ROWS = 8
TILE = 256
FAR = ((0, 16), (16, 16), (32, 32))


def body(
    length_ref, query_ref, count_ref, passages_ref, out_ref,
    held, usable, weights, wide, far_parts, near_parts, own_parts, relay, final, sums,
    near_stat, far_stat,
    load_sem, relay_sem, final_sem, sums_sem, near_sem, far_sem,
):
    gx, gy, gz = lax.axis_index("gx"), lax.axis_index("gy"), lax.axis_index("gz")
    tokens, width = passages_ref.shape[1:]
    queries = query_ref.shape[0]
    share_rows = SHARE * PIECE
    core = lax.rem(gx, 2)
    slot = core * 4 + gz

    def start_of(share):
        offset = jnp.where(share == 2, 2, jnp.where(share == 3, 0, 1 + 2 * share))
        return lax.rem(gz + offset, 4) * share_rows

    def load(share, row, count, sem):
        return pltpu.make_async_copy(
            passages_ref.at[pl.ds(start_of(share) + row, count)],
            held.at[pl.ds(share * share_rows + row, count)], load_sem.at[sem],
        )

    def near_piece(way, n):
        joined, turn = n // 2, n % 2
        return turn + 2 * ((way + joined + 1) % 2)

    def far_load(way, k):
        return load(2, way * HALF + FAR[k][0], FAR[k][1], way * 3 + k)

    def near_load(way, n):
        return load(way, near_piece(way, n) * PIECE, PIECE, 6 + way * SHARE + n)

    def own_load(n):
        return load(3, own_piece(n) * PIECE, PIECE, 14 + n)

    def own_piece(n):
        return (n % 2) * 2 + n // 2

    for k in range(len(FAR)):
        for way in range(2):
            far_load(way, k).start()
    for n in range(SHARE):
        for way in range(2):
            near_load(way, n).start()
    for n in range(SHARE):
        own_load(n).start()

    def near_peer(k):
        to_core = lax.rem(core + k // 4, 2)
        return {"gx": gx - core + to_core, "gz": lax.rem(gz + k % 4, 4)}

    barrier = pltpu.get_barrier_semaphore()
    peers = [{"gy": lax.rem(gy + k, 4)} for k in range(1, 4)]
    peers += [near_peer(k) for k in range(1, 8)]
    peers += [{"gx": lax.rem(gx + 2 * k, 16)} for k in range(1, 8)]
    for peer in peers:
        pl.semaphore_signal(barrier, inc=1, device_id=peer, device_id_type=MESH)

    wide[...] = query_ref[...].reshape(queries * ROWS, width).astype(jnp.float32)
    for i in range(ROWS):
        row = wide[pl.ds(i, queries, stride=ROWS), :]
        weights[:, i * queries : (i + 1) * queries] = row.T.astype(jnp.bfloat16)

    sublane = lax.broadcasted_iota(jnp.int32, (8, TILE), 0)
    odd = [(sublane & k) != 0 for k in (1, 2, 4)]
    token = lax.broadcasted_iota(jnp.int32, (tokens, width), 0)

    def relay_copy(way, k):
        rows = pl.ds(*FAR[k])
        return pltpu.make_async_remote_copy(
            src_ref=far_parts.at[way, rows], dst_ref=relay.at[way, rows],
            send_sem=relay_sem.at[0, way, k], recv_sem=relay_sem.at[1, way, k],
            device_id={"gz": lax.rem(gz + 1 + 2 * way, 4)}, device_id_type=MESH,
        )

    def final_copy(way, piece, source):
        return pltpu.make_async_remote_copy(
            src_ref=source, dst_ref=final.at[way, piece],
            send_sem=final_sem.at[0, way, piece], recv_sem=final_sem.at[1, way, piece],
            device_id={"gz": lax.rem(gz + 1 + 2 * way, 4)}, device_id_type=MESH,
        )

    def sums_copy(k, piece):
        return pltpu.make_async_remote_copy(
            src_ref=sums.at[gy, piece], dst_ref=sums.at[gy, piece],
            send_sem=sums_sem.at[0, k, piece], recv_sem=sums_sem.at[1, k, piece],
            device_id={"gy": lax.rem(gy + k, 4)}, device_id_type=MESH,
        )

    def near_copy(k):
        return pltpu.make_async_remote_copy(
            src_ref=near_stat.at[slot], dst_ref=near_stat.at[slot],
            send_sem=near_sem.at[0, k], recv_sem=near_sem.at[1, k],
            device_id=near_peer(k), device_id_type=MESH,
        )

    def far_copy(k):
        return pltpu.make_async_remote_copy(
            src_ref=far_stat.at[gx // 2], dst_ref=far_stat.at[gx // 2],
            send_sem=far_sem.at[0, k], recv_sem=far_sem.at[1, k],
            device_id={"gx": lax.rem(gx + 2 * k, 16)}, device_id_type=MESH,
        )

    def score(share, row, count, put):
        first = share * share_rows + row
        for group in range(count // 8):
            some = jnp.zeros((8, TILE), jnp.int32)
            for p in range(8):
                at = group * 8 + p
                used = length_ref[start_of(share) + row + at] - gz * tokens
                some = jnp.where(sublane == p, used, some)
                block = held[first + at].astype(jnp.float32)
                block = jnp.where(token < used, block, block[0:1])
                usable[at * tokens : (at + 1) * tokens] = block.astype(jnp.bfloat16)
            any_used = some > 0
            for t in range(ROWS * queries // TILE):
                scores = jnp.dot(
                    usable[group * 8 * tokens : (group + 1) * 8 * tokens],
                    weights[:, t * TILE : (t + 1) * TILE],
                    preferred_element_type=jnp.float32,
                )
                best = []
                for p in range(8):
                    rows = [
                        scores[p * tokens + k : p * tokens + k + 8] for k in range(0, tokens, 8)
                    ]
                    while len(rows) > 1:
                        rows = [jnp.maximum(*rows[k : k + 2]) for k in range(0, len(rows), 2)]
                    best.append(rows[0])
                for level, mask in enumerate(odd):
                    best = [
                        jnp.maximum(
                            jnp.where(mask, b, a),
                            pltpu.roll(jnp.where(mask, a, b), 1 << level, 0),
                        )
                        for a, b in zip(best[::2], best[1::2])
                    ]
                put(group * 8, t, jnp.where(any_used, best[0], masked_low))

    def into(*at):
        def put(row, t, value):
            at[0][(*at[1:-1], pl.ds(at[-1] + row, 8), pl.ds(t * TILE, TILE))] = value

        return put

    for k, (row, count) in enumerate(FAR):
        for way in range(2):
            far_load(way, k).wait()
        for way in range(2):
            score(2, way * HALF + row, count, into(far_parts, way, row))
        if k == 0:
            pl.semaphore_wait(barrier, 17)
        for way in range(2):
            relay_copy(way, k).start()

    def near_step(n, carry):
        for way in range(2):
            near_load(way, n).wait()
        for way in range(2):
            score(way, near_piece(way, n) * PIECE, PIECE, into(near_parts, n, way, 0))

        @pl.when(n == 2)
        def _():
            for way in range(2):
                for k in range(len(FAR)):
                    relay_copy(way, k).wait_recv()

        @pl.when(n >= 2)
        def _():
            rows = pl.ds((n - 2) * PIECE, PIECE)
            for way in range(2):
                near_parts[n, way] = jnp.maximum(near_parts[n, way], relay[way, rows])

        for way in range(2):
            final_copy(way, near_piece(way, n), near_parts.at[n, way]).start()
        return carry

    lax.fori_loop(0, SHARE, near_step, 0)

    def own_step(m, carry):
        for side in range(2):
            own_load(2 * m + side).wait()
        for side in range(2):
            n = 2 * m + side
            score(3, own_piece(n) * PIECE, PIECE, into(own_parts, n, 0))
        return carry

    lax.fori_loop(0, SHARE // 2, own_step, 0)

    def finish(n, carry):
        piece = own_piece(n)
        for way in range(2):
            final_copy(way, piece, own_parts.at[n]).wait_recv()
        total = jnp.zeros((PIECE, queries), jnp.float32)
        for i in range(ROWS):
            lanes = slice(i * queries, (i + 1) * queries)
            best = jnp.maximum(
                own_parts[n, :, lanes],
                jnp.maximum(final[0, piece, :, lanes], final[1, piece, :, lanes]),
            )
            total = total + jnp.where(gy * ROWS + i < count_ref[...], best, 0.0)
        sums[gy, piece] = total
        for k in (2, 1, 3):
            sums_copy(k, piece).start()
        return carry

    lax.fori_loop(0, SHARE, finish, 0)

    for piece in range(SHARE):
        for k in range(1, 4):
            sums_copy(k, piece).wait_recv()
    maxsim = (sums[0] + sums[1]) + (sums[2] + sums[3])
    maxsim = maxsim.reshape(share_rows, queries)

    def joined_stats(stats):
        top = jnp.max(stats, axis=0, keepdims=True)
        return top + jnp.log(jnp.sum(jnp.exp(stats - top), axis=0, keepdims=True))

    near_stat[slot] = joined_stats(maxsim)
    for k in (6, 2, 5, 7, 1, 3, 4):
        near_copy(k).start()
    for k in range(1, 8):
        near_copy(k).wait_recv()
    far_stat[gx // 2] = joined_stats(near_stat[...].reshape(8, queries))
    for k in (4, 3, 5, 2, 6, 1, 7):
        far_copy(k).start()
    for k in range(1, 8):
        far_copy(k).wait_recv()
    norm = joined_stats(far_stat[...].reshape(8, queries))
    out_ref[...] = (maxsim - norm).T

    for way in range(2):
        for k in range(len(FAR)):
            relay_copy(way, k).wait_send()
        for piece in range(SHARE):
            final_copy(way, piece, own_parts.at[0]).wait_send()
    for k in range(1, 4):
        for piece in range(SHARE):
            sums_copy(k, piece).wait_send()
    for k in range(1, 8):
        near_copy(k).wait_send()
        far_copy(k).wait_send()


def shards(queries, passages, passage_len, query_len):
    count, rows, width = queries.shape
    tokens = passages.shape[1]
    f32 = jnp.float32
    vmem = pl.BlockSpec(memory_space=pltpu.VMEM)
    dma = pltpu.SemaphoreType.DMA
    lanes = rows * count
    return pl.pallas_call(
        body,
        out_shape=pltpu.VMEM((count, SHARE * PIECE), f32),
        in_specs=[
            pl.BlockSpec(memory_space=pltpu.SMEM), vmem, vmem, pl.BlockSpec(memory_space=pl.ANY)
        ],
        out_specs=vmem,
        scratch_shapes=[
            pltpu.VMEM(passages.shape, passages.dtype),
            pltpu.VMEM((2 * PIECE * tokens, width), jnp.bfloat16),
            pltpu.VMEM((width, lanes), jnp.bfloat16),
            pltpu.VMEM((lanes, width), f32),
            pltpu.VMEM((2, HALF, lanes), f32),
            pltpu.VMEM((SHARE, 2, PIECE, lanes), f32),
            pltpu.VMEM((SHARE, PIECE, lanes), f32),
            pltpu.VMEM((2, HALF, lanes), f32),
            pltpu.VMEM((2, SHARE, PIECE, lanes), f32),
            pltpu.VMEM((4, SHARE, PIECE, count), f32),
            pltpu.VMEM((8, 1, count), f32),
            pltpu.VMEM((8, 1, count), f32),
            dma((6 + 3 * SHARE,)),
            dma((2, 2, len(FAR))),
            dma((2, 2, SHARE)),
            dma((2, 4, SHARE)),
            dma((2, 8)),
            dma((2, 8)),
        ],
        compiler_params=pltpu.CompilerParams(
            collective_id=0, has_side_effects=True, vmem_limit_bytes=60 * 2**20
        ),
        name="late_interaction",
    )(passage_len, queries, query_len.reshape(1, count), passages)


def solution(mesh):
    return jax.shard_map(
        shards,
        mesh=mesh,
        in_specs=(P(None, "gy", None), P("gx", "gz", None), P("gx"), P()),
        out_specs=P(None, ("gx", "gz")),
        check_vma=False,
    )
```

```python
import jax
import jax.numpy as jnp
from jax import lax
from jax.experimental import pallas as pl
from jax.experimental.pallas import tpu as pltpu
from jax.sharding import PartitionSpec as P

masked_low = -1e30
MESH = pl.DeviceIdType.MESH

PIECE = 32
SHARE = 4
HALF = PIECE * SHARE // 2
ROWS = 8
TILE = 256
FAR = ((0, 16), (16, 16), (32, 32))


def body(
    length_ref, query_ref, count_ref, passages_ref, out_ref,
    held, used_ref, usable, weights, wide, far_parts, near_parts, own_parts, relay, final, sums,
    near_stat, far_stat,
    load_sem, relay_sem, final_sem, sums_sem, near_sem, far_sem,
):
    gx, gy, gz = lax.axis_index("gx"), lax.axis_index("gy"), lax.axis_index("gz")
    tokens, width = passages_ref.shape[1:]
    queries = query_ref.shape[0]
    share_rows = SHARE * PIECE
    core = lax.rem(gx, 2)
    slot = core * 4 + gz

    def start_of(share):
        offset = jnp.where(share == 2, 2, jnp.where(share == 3, 0, 1 + 2 * share))
        return lax.rem(gz + offset, 4) * share_rows

    def load(share, row, count, sem):
        return pltpu.make_async_copy(
            passages_ref.at[pl.ds(start_of(share) + row, count)],
            held.at[pl.ds(share * share_rows + row, count)], load_sem.at[sem],
        )

    def near_piece(way, n):
        joined, turn = n // 2, n % 2
        return turn + 2 * ((way + joined + 1) % 2)

    def far_load(way, k):
        return load(2, way * HALF + FAR[k][0], FAR[k][1], way * 3 + k)

    def near_load(way, n):
        return load(way, near_piece(way, n) * PIECE, PIECE, 6 + way * SHARE + n)

    def own_load(n):
        return load(3, own_piece(n) * PIECE, PIECE, 14 + n)

    def own_piece(n):
        return (n % 2) * 2 + n // 2

    for k in range(len(FAR)):
        for way in range(2):
            far_load(way, k).start()
    for n in range(SHARE):
        for way in range(2):
            near_load(way, n).start()
    for n in range(SHARE):
        own_load(n).start()

    def near_peer(k):
        to_core = lax.rem(core + k // 4, 2)
        return {"gx": gx - core + to_core, "gz": lax.rem(gz + k % 4, 4)}

    barrier = pltpu.get_barrier_semaphore()
    peers = [{"gy": lax.rem(gy + k, 4)} for k in range(1, 4)]
    peers += [near_peer(k) for k in range(1, 8)]
    peers += [{"gx": lax.rem(gx + 2 * k, 16)} for k in range(1, 8)]
    for peer in peers:
        pl.semaphore_signal(barrier, inc=1, device_id=peer, device_id_type=MESH)

    wide[...] = query_ref[...].reshape(queries * ROWS, width).astype(jnp.float32)
    for i in range(ROWS):
        row = wide[pl.ds(i, queries, stride=ROWS), :]
        weights[:, i * queries : (i + 1) * queries] = row.T.astype(jnp.bfloat16)

    for k in range(passages_ref.shape[0] // 128):
        row = length_ref[:, k * 128 : (k + 1) * 128].astype(jnp.float32)
        row = jnp.broadcast_to(row, (128, 128)).T.astype(jnp.int32)
        used_ref[k * 128 : (k + 1) * 128] = row - gz * tokens

    sublane = lax.broadcasted_iota(jnp.int32, (8, TILE), 0)
    odd = [(sublane & k) != 0 for k in (1, 2, 4)]
    token = lax.broadcasted_iota(jnp.int32, (tokens, width), 0)

    def relay_copy(way, k):
        rows = pl.ds(*FAR[k])
        return pltpu.make_async_remote_copy(
            src_ref=far_parts.at[way, rows], dst_ref=relay.at[way, rows],
            send_sem=relay_sem.at[0, way, k], recv_sem=relay_sem.at[1, way, k],
            device_id={"gz": lax.rem(gz + 1 + 2 * way, 4)}, device_id_type=MESH,
        )

    def final_copy(way, piece, source):
        return pltpu.make_async_remote_copy(
            src_ref=source, dst_ref=final.at[way, piece],
            send_sem=final_sem.at[0, way, piece], recv_sem=final_sem.at[1, way, piece],
            device_id={"gz": lax.rem(gz + 1 + 2 * way, 4)}, device_id_type=MESH,
        )

    def sums_copy(k, piece):
        return pltpu.make_async_remote_copy(
            src_ref=sums.at[gy, piece], dst_ref=sums.at[gy, piece],
            send_sem=sums_sem.at[0, k, piece], recv_sem=sums_sem.at[1, k, piece],
            device_id={"gy": lax.rem(gy + k, 4)}, device_id_type=MESH,
        )

    def near_copy(k):
        return pltpu.make_async_remote_copy(
            src_ref=near_stat.at[slot], dst_ref=near_stat.at[slot],
            send_sem=near_sem.at[0, k], recv_sem=near_sem.at[1, k],
            device_id=near_peer(k), device_id_type=MESH,
        )

    def far_copy(k):
        return pltpu.make_async_remote_copy(
            src_ref=far_stat.at[gx // 2], dst_ref=far_stat.at[gx // 2],
            send_sem=far_sem.at[0, k], recv_sem=far_sem.at[1, k],
            device_id={"gx": lax.rem(gx + 2 * k, 16)}, device_id_type=MESH,
        )

    def score(share, row, count, put):
        first = share * share_rows + row
        for group in range(count // 8):
            used = used_ref[pl.ds(pl.multiple_of(start_of(share) + row + group * 8, 8), 8), :]
            for p in range(8):
                at = group * 8 + p
                block = held[first + at]
                usable[at * tokens : (at + 1) * tokens] = jnp.where(
                    token < used[p : p + 1], block, block[0:1]
                )
            any_used = jnp.concatenate([used, used], axis=1) > 0
            for t in range(ROWS * queries // TILE):
                scores = jnp.dot(
                    usable[group * 8 * tokens : (group + 1) * 8 * tokens],
                    weights[:, t * TILE : (t + 1) * TILE],
                    preferred_element_type=jnp.float32,
                )
                best = []
                for p in range(8):
                    rows = [
                        scores[p * tokens + k : p * tokens + k + 8] for k in range(0, tokens, 8)
                    ]
                    while len(rows) > 1:
                        rows = [jnp.maximum(*rows[k : k + 2]) for k in range(0, len(rows), 2)]
                    best.append(rows[0])
                for level, mask in enumerate(odd):
                    best = [
                        jnp.maximum(
                            jnp.where(mask, b, a),
                            pltpu.roll(jnp.where(mask, a, b), 1 << level, 0),
                        )
                        for a, b in zip(best[::2], best[1::2])
                    ]
                put(group * 8, t, jnp.where(any_used, best[0], masked_low))

    def into(*at):
        def put(row, t, value):
            at[0][(*at[1:-1], pl.ds(at[-1] + row, 8), pl.ds(t * TILE, TILE))] = value

        return put

    for k, (row, count) in enumerate(FAR):
        for way in range(2):
            far_load(way, k).wait()
        for way in range(2):
            score(2, way * HALF + row, count, into(far_parts, way, row))
        if k == 0:
            pl.semaphore_wait(barrier, 17)
        for way in range(2):
            relay_copy(way, k).start()

    def near_step(n, carry):
        for way in range(2):
            near_load(way, n).wait()
        for way in range(2):
            score(way, near_piece(way, n) * PIECE, PIECE, into(near_parts, n, way, 0))

        @pl.when(n == 2)
        def _():
            for way in range(2):
                for k in range(len(FAR)):
                    relay_copy(way, k).wait_recv()

        @pl.when(n >= 2)
        def _():
            rows = pl.ds((n - 2) * PIECE, PIECE)
            for way in range(2):
                near_parts[n, way] = jnp.maximum(near_parts[n, way], relay[way, rows])

        for way in range(2):
            final_copy(way, near_piece(way, n), near_parts.at[n, way]).start()
        return carry

    lax.fori_loop(0, SHARE, near_step, 0)

    def own_step(m, carry):
        for side in range(2):
            own_load(2 * m + side).wait()
        for side in range(2):
            n = 2 * m + side
            score(3, own_piece(n) * PIECE, PIECE, into(own_parts, n, 0))
        return carry

    lax.fori_loop(0, SHARE // 2, own_step, 0)

    def finish(n, carry):
        piece = own_piece(n)
        for way in range(2):
            final_copy(way, piece, own_parts.at[n]).wait_recv()
        total = jnp.zeros((PIECE, queries), jnp.float32)
        for i in range(ROWS):
            lanes = slice(i * queries, (i + 1) * queries)
            best = jnp.maximum(
                own_parts[n, :, lanes],
                jnp.maximum(final[0, piece, :, lanes], final[1, piece, :, lanes]),
            )
            total = total + jnp.where(gy * ROWS + i < count_ref[...], best, 0.0)
        sums[gy, piece] = total
        for k in (2, 1, 3):
            sums_copy(k, piece).start()
        return carry

    lax.fori_loop(0, SHARE, finish, 0)

    for piece in range(SHARE):
        for k in range(1, 4):
            sums_copy(k, piece).wait_recv()
    maxsim = (sums[0] + sums[1]) + (sums[2] + sums[3])
    maxsim = maxsim.reshape(share_rows, queries)

    def joined_stats(stats):
        top = jnp.max(stats, axis=0, keepdims=True)
        return top + jnp.log(jnp.sum(jnp.exp(stats - top), axis=0, keepdims=True))

    near_stat[slot] = joined_stats(maxsim)
    for k in (6, 2, 5, 7, 1, 3, 4):
        near_copy(k).start()
    for k in range(1, 8):
        near_copy(k).wait_recv()
    far_stat[gx // 2] = joined_stats(near_stat[...].reshape(8, queries))
    for k in (4, 3, 5, 2, 6, 1, 7):
        far_copy(k).start()
    for k in range(1, 8):
        far_copy(k).wait_recv()
    norm = joined_stats(far_stat[...].reshape(8, queries))
    out_ref[...] = (maxsim - norm).T

    for way in range(2):
        for k in range(len(FAR)):
            relay_copy(way, k).wait_send()
        for piece in range(SHARE):
            final_copy(way, piece, own_parts.at[0]).wait_send()
    for k in range(1, 4):
        for piece in range(SHARE):
            sums_copy(k, piece).wait_send()
    for k in range(1, 8):
        near_copy(k).wait_send()
        far_copy(k).wait_send()


def shards(queries, passages, passage_len, query_len):
    count, rows, width = queries.shape
    tokens = passages.shape[1]
    f32 = jnp.float32
    vmem = pl.BlockSpec(memory_space=pltpu.VMEM)
    dma = pltpu.SemaphoreType.DMA
    lanes = rows * count
    return pl.pallas_call(
        body,
        out_shape=pltpu.VMEM((count, SHARE * PIECE), f32),
        in_specs=[
            vmem, vmem, vmem, pl.BlockSpec(memory_space=pl.ANY)
        ],
        out_specs=vmem,
        scratch_shapes=[
            pltpu.VMEM(passages.shape, passages.dtype),
            pltpu.VMEM((passages.shape[0], 128), jnp.int32),
            pltpu.VMEM((2 * PIECE * tokens, width), jnp.bfloat16),
            pltpu.VMEM((width, lanes), jnp.bfloat16),
            pltpu.VMEM((lanes, width), f32),
            pltpu.VMEM((2, HALF, lanes), f32),
            pltpu.VMEM((SHARE, 2, PIECE, lanes), f32),
            pltpu.VMEM((SHARE, PIECE, lanes), f32),
            pltpu.VMEM((2, HALF, lanes), f32),
            pltpu.VMEM((2, SHARE, PIECE, lanes), f32),
            pltpu.VMEM((4, SHARE, PIECE, count), f32),
            pltpu.VMEM((8, 1, count), f32),
            pltpu.VMEM((8, 1, count), f32),
            dma((6 + 3 * SHARE,)),
            dma((2, 2, len(FAR))),
            dma((2, 2, SHARE)),
            dma((2, 4, SHARE)),
            dma((2, 8)),
            dma((2, 8)),
        ],
        compiler_params=pltpu.CompilerParams(
            collective_id=0, has_side_effects=True, vmem_limit_bytes=60 * 2**20
        ),
        name="late_interaction",
    )(passage_len.reshape(1, -1), queries, query_len.reshape(1, count), passages)


def solution(mesh):
    return jax.shard_map(
        shards,
        mesh=mesh,
        in_specs=(P(None, "gy", None), P("gx", "gz", None), P("gx"), P()),
        out_specs=P(None, ("gx", "gz")),
        check_vma=False,
    )
```

```python
import jax
import jax.numpy as jnp
from jax import lax
from jax.experimental import pallas as pl
from jax.experimental.pallas import tpu as pltpu
from jax.sharding import PartitionSpec as P

masked_low = -1e30
MESH = pl.DeviceIdType.MESH

PIECE = 32
SHARE = 4
HALF = PIECE * SHARE // 2
ROWS = 8
TILE = 256
FAR = ((0, 16), (16, 16), (32, 32))


def body(
    length_ref, query_ref, count_ref, passages_ref, out_ref,
    held, used_ref, usable, weights, wide, far_parts, near_parts, own_parts, relay, final, sums,
    near_stat, far_stat,
    load_sem, relay_sem, final_sem, sums_sem, near_sem, far_sem,
):
    gx, gy, gz = lax.axis_index("gx"), lax.axis_index("gy"), lax.axis_index("gz")
    tokens, width = passages_ref.shape[1:]
    queries = query_ref.shape[0]
    share_rows = SHARE * PIECE
    core = lax.rem(gx, 2)
    slot = core * 4 + gz

    def start_of(share):
        offset = jnp.where(share == 2, 2, jnp.where(share == 3, 0, 1 + 2 * share))
        return lax.rem(gz + offset, 4) * share_rows

    def load(share, row, count, sem):
        return pltpu.make_async_copy(
            passages_ref.at[pl.ds(start_of(share) + row, count)],
            held.at[pl.ds(share * share_rows + row, count)], load_sem.at[sem],
        )

    def near_piece(way, n):
        joined, turn = n // 2, n % 2
        return turn + 2 * ((way + joined + 1) % 2)

    def far_load(way, k):
        return load(2, way * HALF + FAR[k][0], FAR[k][1], way * 3 + k)

    def near_load(way, n):
        return load(way, near_piece(way, n) * PIECE, PIECE, 6 + way * SHARE + n)

    def own_load(n):
        return load(3, own_piece(n) * PIECE, PIECE, 14 + n)

    def own_piece(n):
        return (n % 2) * 2 + n // 2

    for k in range(len(FAR)):
        for way in range(2):
            far_load(way, k).start()
    for n in range(SHARE):
        for way in range(2):
            near_load(way, n).start()
    for n in range(SHARE):
        own_load(n).start()

    def near_peer(k):
        to_core = lax.rem(core + k // 4, 2)
        return {"gx": gx - core + to_core, "gz": lax.rem(gz + k % 4, 4)}

    barrier = pltpu.get_barrier_semaphore()
    peers = [{"gy": lax.rem(gy + k, 4)} for k in range(1, 4)]
    peers += [near_peer(k) for k in range(1, 8)]
    peers += [{"gx": lax.rem(gx + 2 * k, 16)} for k in range(1, 8)]
    for peer in peers:
        pl.semaphore_signal(barrier, inc=1, device_id=peer, device_id_type=MESH)

    wide[...] = query_ref[...].reshape(queries * ROWS, width).astype(jnp.float32)
    for i in range(ROWS):
        row = wide[pl.ds(i, queries, stride=ROWS), :]
        weights[:, i * queries : (i + 1) * queries] = row.T.astype(jnp.bfloat16)

    def lay_out(share):
        rows = pl.ds(pl.multiple_of(start_of(share), share_rows), share_rows)
        row = length_ref[:, rows].astype(jnp.float32)
        row = jnp.broadcast_to(row, (share_rows, 128)).T.astype(jnp.int32)
        used_ref[rows] = row - gz * tokens

    lay_out(2)
    sublane = lax.broadcasted_iota(jnp.int32, (8, TILE), 0)
    odd = [(sublane & k) != 0 for k in (1, 2, 4)]
    token = lax.broadcasted_iota(jnp.int32, (tokens, width), 0)

    def relay_copy(way, k):
        rows = pl.ds(*FAR[k])
        return pltpu.make_async_remote_copy(
            src_ref=far_parts.at[way, rows], dst_ref=relay.at[way, rows],
            send_sem=relay_sem.at[0, way, k], recv_sem=relay_sem.at[1, way, k],
            device_id={"gz": lax.rem(gz + 1 + 2 * way, 4)}, device_id_type=MESH,
        )

    def final_copy(way, piece, source):
        return pltpu.make_async_remote_copy(
            src_ref=source, dst_ref=final.at[way, piece],
            send_sem=final_sem.at[0, way, piece], recv_sem=final_sem.at[1, way, piece],
            device_id={"gz": lax.rem(gz + 1 + 2 * way, 4)}, device_id_type=MESH,
        )

    def sums_copy(k, piece):
        return pltpu.make_async_remote_copy(
            src_ref=sums.at[gy, piece], dst_ref=sums.at[gy, piece],
            send_sem=sums_sem.at[0, k, piece], recv_sem=sums_sem.at[1, k, piece],
            device_id={"gy": lax.rem(gy + k, 4)}, device_id_type=MESH,
        )

    def near_copy(k):
        return pltpu.make_async_remote_copy(
            src_ref=near_stat.at[slot], dst_ref=near_stat.at[slot],
            send_sem=near_sem.at[0, k], recv_sem=near_sem.at[1, k],
            device_id=near_peer(k), device_id_type=MESH,
        )

    def far_copy(k):
        return pltpu.make_async_remote_copy(
            src_ref=far_stat.at[gx // 2], dst_ref=far_stat.at[gx // 2],
            send_sem=far_sem.at[0, k], recv_sem=far_sem.at[1, k],
            device_id={"gx": lax.rem(gx + 2 * k, 16)}, device_id_type=MESH,
        )

    def score(share, row, count, put):
        first = share * share_rows + row
        for group in range(count // 8):
            used = used_ref[pl.ds(pl.multiple_of(start_of(share) + row + group * 8, 8), 8), :]
            for p in range(8):
                at = group * 8 + p
                block = held[first + at]
                usable[at * tokens : (at + 1) * tokens] = jnp.where(
                    token < used[p : p + 1], block, block[0:1]
                )
            any_used = jnp.concatenate([used, used], axis=1) > 0
            for t in range(ROWS * queries // TILE):
                scores = jnp.dot(
                    usable[group * 8 * tokens : (group + 1) * 8 * tokens],
                    weights[:, t * TILE : (t + 1) * TILE],
                    preferred_element_type=jnp.float32,
                )
                best = []
                for p in range(8):
                    rows = [
                        scores[p * tokens + k : p * tokens + k + 8] for k in range(0, tokens, 8)
                    ]
                    while len(rows) > 1:
                        rows = [jnp.maximum(*rows[k : k + 2]) for k in range(0, len(rows), 2)]
                    best.append(rows[0])
                for level, mask in enumerate(odd):
                    best = [
                        jnp.maximum(
                            jnp.where(mask, b, a),
                            pltpu.roll(jnp.where(mask, a, b), 1 << level, 0),
                        )
                        for a, b in zip(best[::2], best[1::2])
                    ]
                put(group * 8, t, jnp.where(any_used, best[0], masked_low))

    def into(*at):
        def put(row, t, value):
            at[0][(*at[1:-1], pl.ds(at[-1] + row, 8), pl.ds(t * TILE, TILE))] = value

        return put

    for k, (row, count) in enumerate(FAR):
        for way in range(2):
            far_load(way, k).wait()
        for way in range(2):
            score(2, way * HALF + row, count, into(far_parts, way, row))
        if k == 0:
            pl.semaphore_wait(barrier, 17)
        for way in range(2):
            relay_copy(way, k).start()
        if k == 0:
            for share in (0, 1, 3):
                lay_out(share)

    def near_step(n, carry):
        for way in range(2):
            near_load(way, n).wait()
        for way in range(2):
            score(way, near_piece(way, n) * PIECE, PIECE, into(near_parts, n, way, 0))

        @pl.when(n == 2)
        def _():
            for way in range(2):
                for k in range(len(FAR)):
                    relay_copy(way, k).wait_recv()

        @pl.when(n >= 2)
        def _():
            rows = pl.ds((n - 2) * PIECE, PIECE)
            for way in range(2):
                near_parts[n, way] = jnp.maximum(near_parts[n, way], relay[way, rows])

        for way in range(2):
            final_copy(way, near_piece(way, n), near_parts.at[n, way]).start()
        return carry

    lax.fori_loop(0, SHARE, near_step, 0)

    def own_step(m, carry):
        for side in range(2):
            own_load(2 * m + side).wait()
        for side in range(2):
            n = 2 * m + side
            score(3, own_piece(n) * PIECE, PIECE, into(own_parts, n, 0))
        return carry

    lax.fori_loop(0, SHARE // 2, own_step, 0)

    def finish(n, carry):
        piece = own_piece(n)
        for way in range(2):
            final_copy(way, piece, own_parts.at[n]).wait_recv()
        total = jnp.zeros((PIECE, queries), jnp.float32)
        for i in range(ROWS):
            lanes = slice(i * queries, (i + 1) * queries)
            best = jnp.maximum(
                own_parts[n, :, lanes],
                jnp.maximum(final[0, piece, :, lanes], final[1, piece, :, lanes]),
            )
            total = total + jnp.where(gy * ROWS + i < count_ref[...], best, 0.0)
        sums[gy, piece] = total
        for k in (2, 1, 3):
            sums_copy(k, piece).start()
        return carry

    lax.fori_loop(0, SHARE, finish, 0)

    for piece in range(SHARE):
        for k in range(1, 4):
            sums_copy(k, piece).wait_recv()
    maxsim = (sums[0] + sums[1]) + (sums[2] + sums[3])
    maxsim = maxsim.reshape(share_rows, queries)

    def joined_stats(stats):
        top = jnp.max(stats, axis=0, keepdims=True)
        return top + jnp.log(jnp.sum(jnp.exp(stats - top), axis=0, keepdims=True))

    near_stat[slot] = joined_stats(maxsim)
    for k in (6, 2, 5, 7, 1, 3, 4):
        near_copy(k).start()
    for k in range(1, 8):
        near_copy(k).wait_recv()
    far_stat[gx // 2] = joined_stats(near_stat[...].reshape(8, queries))
    for k in (4, 3, 5, 2, 6, 1, 7):
        far_copy(k).start()
    for k in range(1, 8):
        far_copy(k).wait_recv()
    norm = joined_stats(far_stat[...].reshape(8, queries))
    out_ref[...] = (maxsim - norm).T

    for way in range(2):
        for k in range(len(FAR)):
            relay_copy(way, k).wait_send()
        for piece in range(SHARE):
            final_copy(way, piece, own_parts.at[0]).wait_send()
    for k in range(1, 4):
        for piece in range(SHARE):
            sums_copy(k, piece).wait_send()
    for k in range(1, 8):
        near_copy(k).wait_send()
        far_copy(k).wait_send()


def shards(queries, passages, passage_len, query_len):
    count, rows, width = queries.shape
    tokens = passages.shape[1]
    f32 = jnp.float32
    vmem = pl.BlockSpec(memory_space=pltpu.VMEM)
    dma = pltpu.SemaphoreType.DMA
    lanes = rows * count
    return pl.pallas_call(
        body,
        out_shape=pltpu.VMEM((count, SHARE * PIECE), f32),
        in_specs=[
            vmem, vmem, vmem, pl.BlockSpec(memory_space=pl.ANY)
        ],
        out_specs=vmem,
        scratch_shapes=[
            pltpu.VMEM(passages.shape, passages.dtype),
            pltpu.VMEM((passages.shape[0], 128), jnp.int32),
            pltpu.VMEM((2 * PIECE * tokens, width), jnp.bfloat16),
            pltpu.VMEM((width, lanes), jnp.bfloat16),
            pltpu.VMEM((lanes, width), f32),
            pltpu.VMEM((2, HALF, lanes), f32),
            pltpu.VMEM((SHARE, 2, PIECE, lanes), f32),
            pltpu.VMEM((SHARE, PIECE, lanes), f32),
            pltpu.VMEM((2, HALF, lanes), f32),
            pltpu.VMEM((2, SHARE, PIECE, lanes), f32),
            pltpu.VMEM((4, SHARE, PIECE, count), f32),
            pltpu.VMEM((8, 1, count), f32),
            pltpu.VMEM((8, 1, count), f32),
            dma((6 + 3 * SHARE,)),
            dma((2, 2, len(FAR))),
            dma((2, 2, SHARE)),
            dma((2, 4, SHARE)),
            dma((2, 8)),
            dma((2, 8)),
        ],
        compiler_params=pltpu.CompilerParams(
            collective_id=0, has_side_effects=True, vmem_limit_bytes=60 * 2**20
        ),
        name="late_interaction",
    )(passage_len.reshape(1, -1), queries, query_len.reshape(1, count), passages)


def solution(mesh):
    return jax.shard_map(
        shards,
        mesh=mesh,
        in_specs=(P(None, "gy", None), P("gx", "gz", None), P("gx"), P()),
        out_specs=P(None, ("gx", "gz")),
        check_vma=False,
    )
```

```python
import jax
import jax.numpy as jnp
from jax import lax
from jax.experimental import pallas as pl
from jax.experimental.pallas import tpu as pltpu
from jax.sharding import PartitionSpec as P

masked_low = -1e30
MESH = pl.DeviceIdType.MESH

PIECE = 32
SHARE = 4
HALF = PIECE * SHARE // 2
ROWS = 8
TILE = 256
FAR = ((0, 16), (16, 24), (40, 24))


def body(
    length_ref, query_ref, count_ref, passages_ref, out_ref,
    held, used_ref, usable, weights, wide, far_parts, near_parts, own_parts, relay, final, sums,
    near_stat, far_stat,
    load_sem, relay_sem, final_sem, sums_sem, near_sem, far_sem,
):
    gx, gy, gz = lax.axis_index("gx"), lax.axis_index("gy"), lax.axis_index("gz")
    tokens, width = passages_ref.shape[1:]
    queries = query_ref.shape[0]
    share_rows = SHARE * PIECE
    core = lax.rem(gx, 2)
    slot = core * 4 + gz

    def start_of(share):
        offset = jnp.where(share == 2, 2, jnp.where(share == 3, 0, 1 + 2 * share))
        return lax.rem(gz + offset, 4) * share_rows

    def load(share, row, count, sem):
        return pltpu.make_async_copy(
            passages_ref.at[pl.ds(start_of(share) + row, count)],
            held.at[pl.ds(share * share_rows + row, count)], load_sem.at[sem],
        )

    def near_piece(way, n):
        joined, turn = n // 2, n % 2
        return turn + 2 * ((way + joined + 1) % 2)

    def far_load(way, k):
        return load(2, way * HALF + FAR[k][0], FAR[k][1], way * 3 + k)

    def near_load(way, n):
        return load(way, near_piece(way, n) * PIECE, PIECE, 6 + way * SHARE + n)

    def own_load(n):
        return load(3, own_piece(n) * PIECE, PIECE, 14 + n)

    def own_piece(n):
        return (n % 2) * 2 + n // 2

    for k in range(len(FAR)):
        for way in range(2):
            far_load(way, k).start()
    for n in range(SHARE):
        for way in range(2):
            near_load(way, n).start()
    for n in range(SHARE):
        own_load(n).start()

    def near_peer(k):
        to_core = lax.rem(core + k // 4, 2)
        return {"gx": gx - core + to_core, "gz": lax.rem(gz + k % 4, 4)}

    barrier = pltpu.get_barrier_semaphore()
    peers = [{"gy": lax.rem(gy + k, 4)} for k in range(1, 4)]
    peers += [near_peer(k) for k in range(1, 8)]
    peers += [{"gx": lax.rem(gx + 2 * k, 16)} for k in range(1, 8)]
    for peer in peers:
        pl.semaphore_signal(barrier, inc=1, device_id=peer, device_id_type=MESH)

    wide[...] = query_ref[...].reshape(queries * ROWS, width).astype(jnp.float32)
    for i in range(ROWS):
        row = wide[pl.ds(i, queries, stride=ROWS), :]
        weights[:, i * queries : (i + 1) * queries] = row.T.astype(jnp.bfloat16)

    for k in range(passages_ref.shape[0] // 128):
        row = length_ref[:, k * 128 : (k + 1) * 128].astype(jnp.float32)
        row = jnp.broadcast_to(row, (128, 128)).T.astype(jnp.int32)
        used_ref[k * 128 : (k + 1) * 128] = row - gz * tokens

    sublane = lax.broadcasted_iota(jnp.int32, (8, TILE), 0)
    odd = [(sublane & k) != 0 for k in (1, 2, 4)]
    token = lax.broadcasted_iota(jnp.int32, (tokens, width), 0)

    def relay_copy(way, k):
        rows = pl.ds(*FAR[k])
        return pltpu.make_async_remote_copy(
            src_ref=far_parts.at[way, rows], dst_ref=relay.at[way, rows],
            send_sem=relay_sem.at[0, way, k], recv_sem=relay_sem.at[1, way, k],
            device_id={"gz": lax.rem(gz + 1 + 2 * way, 4)}, device_id_type=MESH,
        )

    def final_copy(way, piece, source):
        return pltpu.make_async_remote_copy(
            src_ref=source, dst_ref=final.at[way, piece],
            send_sem=final_sem.at[0, way, piece], recv_sem=final_sem.at[1, way, piece],
            device_id={"gz": lax.rem(gz + 1 + 2 * way, 4)}, device_id_type=MESH,
        )

    def sums_copy(k, piece):
        return pltpu.make_async_remote_copy(
            src_ref=sums.at[gy, piece], dst_ref=sums.at[gy, piece],
            send_sem=sums_sem.at[0, k, piece], recv_sem=sums_sem.at[1, k, piece],
            device_id={"gy": lax.rem(gy + k, 4)}, device_id_type=MESH,
        )

    def near_copy(k):
        return pltpu.make_async_remote_copy(
            src_ref=near_stat.at[slot], dst_ref=near_stat.at[slot],
            send_sem=near_sem.at[0, k], recv_sem=near_sem.at[1, k],
            device_id=near_peer(k), device_id_type=MESH,
        )

    def far_copy(k):
        return pltpu.make_async_remote_copy(
            src_ref=far_stat.at[gx // 2], dst_ref=far_stat.at[gx // 2],
            send_sem=far_sem.at[0, k], recv_sem=far_sem.at[1, k],
            device_id={"gx": lax.rem(gx + 2 * k, 16)}, device_id_type=MESH,
        )

    def score(share, row, count, put):
        first = share * share_rows + row
        for group in range(count // 8):
            used = used_ref[pl.ds(pl.multiple_of(start_of(share) + row + group * 8, 8), 8), :]
            for p in range(8):
                at = group * 8 + p
                block = held[first + at]
                usable[at * tokens : (at + 1) * tokens] = jnp.where(
                    token < used[p : p + 1], block, block[0:1]
                )
            any_used = jnp.concatenate([used, used], axis=1) > 0
            for t in range(ROWS * queries // TILE):
                scores = jnp.dot(
                    usable[group * 8 * tokens : (group + 1) * 8 * tokens],
                    weights[:, t * TILE : (t + 1) * TILE],
                    preferred_element_type=jnp.float32,
                )
                best = []
                for p in range(8):
                    rows = [
                        scores[p * tokens + k : p * tokens + k + 8] for k in range(0, tokens, 8)
                    ]
                    while len(rows) > 1:
                        rows = [jnp.maximum(*rows[k : k + 2]) for k in range(0, len(rows), 2)]
                    best.append(rows[0])
                for level, mask in enumerate(odd):
                    best = [
                        jnp.maximum(
                            jnp.where(mask, b, a),
                            pltpu.roll(jnp.where(mask, a, b), 1 << level, 0),
                        )
                        for a, b in zip(best[::2], best[1::2])
                    ]
                put(group * 8, t, jnp.where(any_used, best[0], masked_low))

    def into(*at):
        def put(row, t, value):
            at[0][(*at[1:-1], pl.ds(at[-1] + row, 8), pl.ds(t * TILE, TILE))] = value

        return put

    for k, (row, count) in enumerate(FAR):
        for way in range(2):
            far_load(way, k).wait()
        for way in range(2):
            score(2, way * HALF + row, count, into(far_parts, way, row))
        if k == 0:
            pl.semaphore_wait(barrier, 17)
        for way in range(2):
            relay_copy(way, k).start()

    def near_step(n, carry):
        for way in range(2):
            near_load(way, n).wait()
        for way in range(2):
            score(way, near_piece(way, n) * PIECE, PIECE, into(near_parts, n, way, 0))

        @pl.when(n == 2)
        def _():
            for way in range(2):
                for k in range(len(FAR)):
                    relay_copy(way, k).wait_recv()

        @pl.when(n >= 2)
        def _():
            rows = pl.ds((n - 2) * PIECE, PIECE)
            for way in range(2):
                near_parts[n, way] = jnp.maximum(near_parts[n, way], relay[way, rows])

        for way in range(2):
            final_copy(way, near_piece(way, n), near_parts.at[n, way]).start()
        return carry

    lax.fori_loop(0, SHARE, near_step, 0)

    def own_step(m, carry):
        for side in range(2):
            own_load(2 * m + side).wait()
        for side in range(2):
            n = 2 * m + side
            score(3, own_piece(n) * PIECE, PIECE, into(own_parts, n, 0))
        return carry

    lax.fori_loop(0, SHARE // 2, own_step, 0)

    def finish(n, carry):
        piece = own_piece(n)
        for way in range(2):
            final_copy(way, piece, own_parts.at[n]).wait_recv()
        total = jnp.zeros((PIECE, queries), jnp.float32)
        for i in range(ROWS):
            lanes = slice(i * queries, (i + 1) * queries)
            best = jnp.maximum(
                own_parts[n, :, lanes],
                jnp.maximum(final[0, piece, :, lanes], final[1, piece, :, lanes]),
            )
            total = total + jnp.where(gy * ROWS + i < count_ref[...], best, 0.0)
        sums[gy, piece] = total
        for k in (2, 1, 3):
            sums_copy(k, piece).start()
        return carry

    lax.fori_loop(0, SHARE, finish, 0)

    for piece in range(SHARE):
        for k in range(1, 4):
            sums_copy(k, piece).wait_recv()
    maxsim = (sums[0] + sums[1]) + (sums[2] + sums[3])
    maxsim = maxsim.reshape(share_rows, queries)

    def joined_stats(stats):
        top = jnp.max(stats, axis=0, keepdims=True)
        return top + jnp.log(jnp.sum(jnp.exp(stats - top), axis=0, keepdims=True))

    near_stat[slot] = joined_stats(maxsim)
    for k in (6, 2, 5, 7, 1, 3, 4):
        near_copy(k).start()
    for k in range(1, 8):
        near_copy(k).wait_recv()
    far_stat[gx // 2] = joined_stats(near_stat[...].reshape(8, queries))
    for k in (4, 3, 5, 2, 6, 1, 7):
        far_copy(k).start()
    for k in range(1, 8):
        far_copy(k).wait_recv()
    norm = joined_stats(far_stat[...].reshape(8, queries))
    out_ref[...] = (maxsim - norm).T

    for way in range(2):
        for k in range(len(FAR)):
            relay_copy(way, k).wait_send()
        for piece in range(SHARE):
            final_copy(way, piece, own_parts.at[0]).wait_send()
    for k in range(1, 4):
        for piece in range(SHARE):
            sums_copy(k, piece).wait_send()
    for k in range(1, 8):
        near_copy(k).wait_send()
        far_copy(k).wait_send()


def shards(queries, passages, passage_len, query_len):
    count, rows, width = queries.shape
    tokens = passages.shape[1]
    f32 = jnp.float32
    vmem = pl.BlockSpec(memory_space=pltpu.VMEM)
    dma = pltpu.SemaphoreType.DMA
    lanes = rows * count
    return pl.pallas_call(
        body,
        out_shape=pltpu.VMEM((count, SHARE * PIECE), f32),
        in_specs=[
            vmem, vmem, vmem, pl.BlockSpec(memory_space=pl.ANY)
        ],
        out_specs=vmem,
        scratch_shapes=[
            pltpu.VMEM(passages.shape, passages.dtype),
            pltpu.VMEM((passages.shape[0], 128), jnp.int32),
            pltpu.VMEM((2 * PIECE * tokens, width), jnp.bfloat16),
            pltpu.VMEM((width, lanes), jnp.bfloat16),
            pltpu.VMEM((lanes, width), f32),
            pltpu.VMEM((2, HALF, lanes), f32),
            pltpu.VMEM((SHARE, 2, PIECE, lanes), f32),
            pltpu.VMEM((SHARE, PIECE, lanes), f32),
            pltpu.VMEM((2, HALF, lanes), f32),
            pltpu.VMEM((2, SHARE, PIECE, lanes), f32),
            pltpu.VMEM((4, SHARE, PIECE, count), f32),
            pltpu.VMEM((8, 1, count), f32),
            pltpu.VMEM((8, 1, count), f32),
            dma((6 + 3 * SHARE,)),
            dma((2, 2, len(FAR))),
            dma((2, 2, SHARE)),
            dma((2, 4, SHARE)),
            dma((2, 8)),
            dma((2, 8)),
        ],
        compiler_params=pltpu.CompilerParams(
            collective_id=0, has_side_effects=True, vmem_limit_bytes=60 * 2**20
        ),
        name="late_interaction",
    )(passage_len.reshape(1, -1), queries, query_len.reshape(1, count), passages)


def solution(mesh):
    return jax.shard_map(
        shards,
        mesh=mesh,
        in_specs=(P(None, "gy", None), P("gx", "gz", None), P("gx"), P()),
        out_specs=P(None, ("gx", "gz")),
        check_vma=False,
    )
```
